32 devices in a mesh: south: 2 (over x), east: 4 (over y, core), down: 4 (over z).
Axes of the slice: x: 2, y: 2, z: 4, core: 2. Of those that a mesh axis runs over, the one named last changes fastest.
Arguments:
- field_values: float32 [256, 32, 32, 128], P('south', 'east', 'down'), may hold values from 0.5 to 2
- flow_j: float32 [256, 32, 32, 128], P('south', 'east', 'down'), may hold values from -0.3 to 0.3
- flow_i: float32 [256, 32, 32, 128], P('south', 'east', 'down'), may hold values from -0.3 to 0.3
- flow_k: float32 [256, 32, 32, 128], P('south', 'east', 'down'), may hold values from -0.3 to 0.3
Outputs:
- standardized: float32 [256, 32, 32, 128], P('south', 'east', 'down')
- field_values_end: float32 [256, 32, 32, 128], P('south', 'east', 'down')
The draws below stay inside these ranges and needn't reach their ends.
All inputs are finite; a program needn't handle non-finite values.
Results may differ from the reference program's by a relative error of at most 0.00002.
Values sent between devices are 32-bit elements; how exact they have to be, the bound alone decides.
A program may use at most 128 MiB of HBM per device.

```python
import jax
import jax.numpy as jnp
from jax import lax

GRID_J = 256
GRID_I = 32
GRID_K = 32
LEVELS = 128
STEPS = 6


def block_scale(key, shape, cuts, smallest, high):
    def one(dim, blocks):
        steps = jax.random.uniform(jax.random.fold_in(jax.random.fold_in(key, 6), dim), (blocks,), jnp.float32, smallest / len(cuts), high / len(cuts))
        return jnp.repeat(jnp.exp(steps), shape[dim] // blocks).reshape((-1,) + (1,) * (len(shape) - dim - 1))

    level = one(*cuts[0])
    for cut in cuts[1:]:
        level = level * one(*cut)
    return level


def setup_inputs(seed: int = 0) -> dict:
    key_of = jax.random.split(jax.random.key(seed), 5)
    return {
        "field_values": jnp.clip(0.5 + 1.5 * jax.random.uniform(key_of[0], (GRID_J, GRID_I, GRID_K, LEVELS), jnp.float32) ** block_scale(key_of[0], (GRID_J, GRID_I, GRID_K, LEVELS), ((0, 2), (1, 4), (2, 4)), -0.2, 0.2), 0.5, 2.0),
        "flow_j": jnp.clip(jax.random.uniform(key_of[1], (GRID_J, GRID_I, GRID_K, LEVELS), jnp.float32, -0.3, 0.3) * block_scale(key_of[1], (GRID_J, GRID_I, GRID_K, LEVELS), ((0, 2), (1, 4), (2, 4)), -0.4, 0.0), -0.3, 0.3),
        "flow_i": jnp.clip(jax.random.uniform(key_of[2], (GRID_J, GRID_I, GRID_K, LEVELS), jnp.float32, -0.3, 0.3) * block_scale(key_of[2], (GRID_J, GRID_I, GRID_K, LEVELS), ((0, 2), (1, 4), (2, 4)), -0.4, 0.0), -0.3, 0.3),
        "flow_k": jnp.clip(jax.random.uniform(key_of[3], (GRID_J, GRID_I, GRID_K, LEVELS), jnp.float32, -0.3, 0.3) * block_scale(key_of[3], (GRID_J, GRID_I, GRID_K, LEVELS), ((0, 2), (1, 4), (2, 4)), -0.4, 0.0), -0.3, 0.3),
    }


def inner_cells(values, dims):
    for dim in dims:
        values = lax.slice_in_dim(values, 1, values.shape[dim] - 1, axis=dim)
    return values

def side_cells(values, dim, start, dims):
    others = [other for other in dims if other != dim]
    values = inner_cells(values, others)
    return lax.slice_in_dim(values, start, start + values.shape[dim] - 2, axis=dim)

def advance(padded, flow_j, flow_i, flow_k):
    middle = inner_cells(padded, (0, 1, 2))
    lower = [side_cells(padded, dim, 0, (0, 1, 2)) for dim in (0, 1, 2)]
    upper = [side_cells(padded, dim, 2, (0, 1, 2)) for dim in (0, 1, 2)]
    slopes = [above - below for above, below in zip(upper, lower)]
    smooth_rate = 0.05
    spread = lower[0] + upper[0] + lower[1] + upper[1] + lower[2] + upper[2] - 6.0 * middle
    return middle - flow_j * slopes[0] - flow_i * slopes[1] - flow_k * slopes[2] + smooth_rate * spread

def reference(field_values, flow_j, flow_i, flow_k):
    for step in range(STEPS):
        field_values = advance(jnp.pad(field_values, ((1, 1), (1, 1), (1, 1), (0, 0)), mode='constant'), flow_j, flow_i, flow_k)
    line_mean = lax.optimization_barrier(jnp.mean(field_values, axis=0, keepdims=True))
    centred = field_values - line_mean
    line_variance = lax.optimization_barrier(jnp.mean(centred * centred, axis=0, keepdims=True))
    standardized = centred * lax.rsqrt(line_variance + 0.0001)
    return (standardized, field_values)
```

```python
import functools

import jax
import jax.numpy as jnp
from jax import lax
from jax.experimental import pallas as pl
from jax.experimental.pallas import tpu as pltpu
from jax.sharding import PartitionSpec as P

STEPS = 6
PIECES = 8
MESH = pl.DeviceIdType.MESH


def transport(counts, pieces, steps, field, flow_j, flow_i, flow_k, end, mean_out, scale_out,
              cells, flows, face_out, face_in, stats,
              load_sem, flow_sem, end_sem, k_send, k_recv, i_send, i_recv, j_send, j_recv,
              stat_send, stat_recv):
    n_south, n_east, n_down = counts
    nj, ni, nk, _ = field.shape
    rows = nj // pieces
    south, east, down = (lax.axis_index(a) for a in ("south", "east", "down"))
    place = {"south": (south, n_south), "east": (east, n_east), "down": (down, n_down)}
    downward = lax.rem(south, 2) == 0

    def has(axis, side):
        me, count = place[axis]
        return me > 0 if side == 0 else me < count - 1

    def beside(axis, side):
        me, _ = place[axis]
        return {axis: me - 1 if side == 0 else me + 1}

    def piece_of(c):
        return jnp.where(downward, pieces - 1 - c, c)

    def load(c):
        return pltpu.make_async_copy(
            field.at[pl.ds(c * rows, rows)],
            cells.at[0, pl.ds(c * rows + 1, rows), pl.ds(1, ni)],
            load_sem.at[c],
        )

    def load_flow(d, c):
        source = (flow_j, flow_i, flow_k)[d]
        part = pl.ds(c * rows, rows)
        return pltpu.make_async_copy(source.at[part], flows.at[d, part], flow_sem.at[d, c])

    def k_copy(slot, side, c):
        part = pl.ds(c * rows, rows)
        return pltpu.make_async_remote_copy(
            face_out.at[slot, side, part], face_in.at[slot, 1 - side, part],
            k_send.at[slot, side, c], k_recv.at[slot, 1 - side, c],
            device_id=beside("down", side), device_id_type=MESH,
        )

    def i_copy(slot, side, c):
        part = pl.ds(c * rows + 1, rows)
        return pltpu.make_async_remote_copy(
            cells.at[slot, part, 1 if side == 0 else ni],
            cells.at[slot, part, ni + 1 if side == 0 else 0],
            i_send.at[slot, side, c], i_recv.at[slot, 1 - side, c],
            device_id=beside("east", side), device_id_type=MESH,
        )

    def j_copy(slot, side):
        return pltpu.make_async_remote_copy(
            cells.at[slot, 1 if side == 0 else nj, pl.ds(1, ni)],
            cells.at[slot, nj + 1 if side == 0 else 0, pl.ds(1, ni)],
            j_send.at[slot, side], j_recv.at[slot, 1 - side],
            device_id=beside("south", side), device_id_type=MESH,
        )

    def each_copy(slot, c, act):
        for side in (0, 1):
            pl.when(has("down", side))(lambda: act(k_copy(slot, side, c), side))
        for side in (0, 1):
            pl.when(has("east", side))(lambda: act(i_copy(slot, side, c), side))
        for side in (0, 1):
            edge = 0 if side == 0 else pieces - 1
            pl.when(has("south", side) & (c == edge))(lambda: act(j_copy(slot, side), side))

    def send(slot, c):
        each_copy(slot, c, lambda copy, side: copy.start())

    def sent(slot, c):
        each_copy(slot, c, lambda copy, side: copy.wait_send())

    def received(slot, c):
        for side in (0, 1):
            pl.when(has("down", side))(lambda: k_copy(slot, 1 - side, c).wait_recv())
        for side in (0, 1):
            pl.when(has("east", side))(lambda: i_copy(slot, 1 - side, c).wait_recv())
        for side in (0, 1):
            edge = 0 if side == 0 else pieces - 1
            pl.when(has("south", side) & (c == edge))(
                lambda: j_copy(slot, 1 - side).wait_recv()
            )

    @pl.loop(0, pieces)
    def _(c):
        load(piece_of(c)).start()

    @pl.loop(0, pieces)
    def _(c):
        for d in range(3):
            load_flow(d, piece_of(c)).start()

    barrier = pltpu.get_barrier_semaphore()
    for axis in ("east", "down"):
        for side in (0, 1):
            @pl.when(has(axis, side))
            def _():
                pl.semaphore_signal(barrier, 1, device_id=beside(axis, side), device_id_type=MESH)
    for offset in range(1, n_south):
        other = {"south": lax.rem(south + offset, n_south)}
        pl.semaphore_signal(barrier, 1, device_id=other, device_id_type=MESH)

    for side in (0, 1):
        @pl.when(jnp.logical_not(has("down", side)))
        def _():
            @pl.loop(0, nj)
            def _(r):
                for slot in (0, 1):
                    face_in[slot, side, r] = jnp.zeros(face_in.shape[3:], jnp.float32)

        @pl.when(jnp.logical_not(has("east", side)))
        def _():
            @pl.loop(0, nj)
            def _(r):
                for slot in (0, 1):
                    cells[slot, r + 1, 0 if side == 0 else ni + 1] = jnp.zeros(
                        cells.shape[3:], jnp.float32)

        @pl.when(jnp.logical_not(has("south", side)))
        def _():
            for slot in (0, 1):
                cells[slot, 0 if side == 0 else nj + 1, pl.ds(1, ni)] = jnp.zeros(
                    field.shape[1:], jnp.float32)

    peers = n_south - 1
    for axis in ("east", "down"):
        for side in (0, 1):
            peers = peers + has(axis, side).astype(jnp.int32)
    pl.semaphore_wait(barrier, peers)

    @pl.loop(0, pieces)
    def _(index):
        c = piece_of(index)
        load(c).wait()

        @pl.loop(0, rows)
        def _(offset):
            r = c * rows + offset
            values = cells[0, r + 1, pl.ds(1, ni)]
            face_out[0, 0, r] = values[:, 0, :]
            face_out[0, 1, r] = values[:, nk - 1, :]

        send(0, c)

    height = lax.broadcasted_iota(jnp.int32, field.shape[1:], 1)

    def advanced(slot, r):
        middle = cells[slot, r + 1, pl.ds(1, ni)]
        j_low = cells[slot, r, pl.ds(1, ni)]
        j_high = cells[slot, r + 2, pl.ds(1, ni)]
        i_low = cells[slot, r + 1, pl.ds(0, ni)]
        i_high = cells[slot, r + 1, pl.ds(2, ni)]
        k_low = jnp.where(
            height == 0, face_in[slot, 0, r][:, None, :], pltpu.roll(middle, 1, 1))
        k_high = jnp.where(
            height == nk - 1, face_in[slot, 1, r][:, None, :], pltpu.roll(middle, nk - 1, 1))
        spread = (j_low + j_high) + (i_low + i_high) + (k_low + k_high) - 6.0 * middle
        drift = (flows[0, r] * (j_high - j_low) + flows[1, r] * (i_high - i_low)
                 + flows[2, r] * (k_high - k_low))
        return middle - drift + 0.05 * spread

    @pl.loop(1, steps)
    def _(step):
        now, later = lax.rem(step + 1, 2), lax.rem(step, 2)

        @pl.loop(0, pieces)
        def _(index):
            c = piece_of(index)

            @pl.when(step == 1)
            def _():
                for d in range(3):
                    load_flow(d, c).wait()

            @pl.when(step >= 2)
            def _():
                sent(later, c)

            received(now, c)

            @pl.loop(0, rows)
            def _(offset):
                r = c * rows + offset
                values = advanced(now, r)
                cells[later, r + 1, pl.ds(1, ni)] = values
                face_out[later, 0, r] = values[:, 0, :]
                face_out[later, 1, r] = values[:, nk - 1, :]

            send(later, c)

    now, later = (steps - 1) % 2, steps % 2

    def store(c):
        return pltpu.make_async_copy(
            cells.at[later, pl.ds(c * rows + 1, rows), pl.ds(1, ni)],
            end.at[pl.ds(c * rows, rows)],
            end_sem.at[c],
        )

    def finish(index, total):
        c = piece_of(index)
        sent(later, c)
        received(now, c)

        def row(offset, total):
            r = c * rows + offset
            values = advanced(now, r)
            cells[later, r + 1, pl.ds(1, ni)] = values
            return total + values

        total = lax.fori_loop(0, rows, row, total)
        store(c).start()
        return total

    zero = jnp.zeros(field.shape[1:], jnp.float32)
    mean = lax.fori_loop(0, pieces, finish, zero) * (1.0 / nj)

    def square(r, total):
        centred = cells[later, r + 1, pl.ds(1, ni)] - mean
        return total + centred * centred

    squares = lax.fori_loop(0, nj, square, zero)
    stats[south, 0] = mean
    stats[south, 1] = squares

    def stat_copy(offset, owner):
        target = lax.rem(south + offset, n_south)
        return pltpu.make_async_remote_copy(
            stats.at[owner], stats.at[owner], stat_send.at[offset - 1], stat_recv.at[offset - 1],
            device_id={"south": target}, device_id_type=MESH,
        )

    for offset in range(1, n_south):
        stat_copy(offset, south).start()

    @pl.loop(0, pieces)
    def _(c):
        sent(now, c)
        store(c).wait()

    for offset in range(1, n_south):
        owner = lax.rem(south + n_south - offset, n_south)
        stat_copy(offset, owner).wait_recv()
    whole_mean = stats[0, 0]
    for other in range(1, n_south):
        whole_mean = whole_mean + stats[other, 0]
    whole_mean = whole_mean * (1.0 / n_south)
    whole_squares = zero
    for other in range(n_south):
        away = stats[other, 0] - whole_mean
        whole_squares = whole_squares + (stats[other, 1] + nj * (away * away))
    mean_out[...] = whole_mean
    scale_out[...] = lax.rsqrt(whole_squares * (1.0 / (nj * n_south)) + 0.0001)
    for offset in range(1, n_south):
        stat_copy(offset, south).wait_send()


def scale(values, mean, factor, standardized, copied):
    block = values[...]
    copied[...] = block
    standardized[...] = (block - mean[...][None]) * factor[...][None]


def per_device(counts, field_values, flow_j, flow_i, flow_k):
    nj, ni, nk, levels = field_values.shape
    pieces = PIECES
    n_south = counts[0]
    plane = (ni, nk, levels)
    end, mean, factor = pl.pallas_call(
        functools.partial(transport, counts, pieces, STEPS),
        name="transport",
        out_shape=(
            jax.ShapeDtypeStruct(field_values.shape, jnp.float32),
            jax.ShapeDtypeStruct(plane, jnp.float32),
            jax.ShapeDtypeStruct(plane, jnp.float32),
        ),
        in_specs=[pl.BlockSpec(memory_space=pltpu.HBM)] * 4,
        out_specs=(
            pl.BlockSpec(memory_space=pl.ANY),
            pl.BlockSpec(memory_space=pltpu.VMEM),
            pl.BlockSpec(memory_space=pltpu.VMEM),
        ),
        scratch_shapes=[
            pltpu.VMEM((2, nj + 2, ni + 2, nk, levels), jnp.float32),
            pltpu.VMEM((3,) + field_values.shape, jnp.float32),
            pltpu.VMEM((2, 2, nj, ni, levels), jnp.float32),
            pltpu.VMEM((2, 2, nj, ni, levels), jnp.float32),
            pltpu.VMEM((n_south, 2) + plane, jnp.float32),
            pltpu.SemaphoreType.DMA((pieces,)),
            pltpu.SemaphoreType.DMA((3, pieces)),
            pltpu.SemaphoreType.DMA((pieces,)),
            pltpu.SemaphoreType.DMA((2, 2, pieces)),
            pltpu.SemaphoreType.DMA((2, 2, pieces)),
            pltpu.SemaphoreType.DMA((2, 2, pieces)),
            pltpu.SemaphoreType.DMA((2, 2, pieces)),
            pltpu.SemaphoreType.DMA((2, 2)),
            pltpu.SemaphoreType.DMA((2, 2)),
            pltpu.SemaphoreType.DMA((max(n_south - 1, 1),)),
            pltpu.SemaphoreType.DMA((max(n_south - 1, 1),)),
        ],
        compiler_params=pltpu.CompilerParams(
            collective_id=0, has_side_effects=True, vmem_limit_bytes=34 * 2**20
        ),
    )(*(pltpu.with_memory_space_constraint(array, pltpu.HBM)
        for array in (field_values, flow_j, flow_i, flow_k)))
    rows = nj // pieces
    block = pl.BlockSpec((rows,) + plane, lambda c: (c, 0, 0, 0))
    flat = pl.BlockSpec(plane, lambda c: (0, 0, 0))
    return pl.pallas_call(
        scale,
        name="scale",
        grid=(nj // rows,),
        in_specs=[block, flat, flat],
        out_specs=(block, block),
        out_shape=(jax.ShapeDtypeStruct(field_values.shape, jnp.float32),) * 2,
        compiler_params=pltpu.CompilerParams(vmem_limit_bytes=16 * 2**20),
    )(end, mean, factor)


def solution(mesh):
    counts = tuple(mesh.shape[axis] for axis in ("south", "east", "down"))
    spec = P("south", "east", "down", None)
    return jax.shard_map(
        functools.partial(per_device, counts),
        mesh=mesh,
        in_specs=(spec,) * 4,
        out_specs=(spec, spec),
        check_vma=False,
    )
```

```python
import functools

import jax
import jax.numpy as jnp
from jax import lax
from jax.experimental import pallas as pl
from jax.experimental.pallas import tpu as pltpu
from jax.sharding import PartitionSpec as P

STEPS = 6
PIECES = 8
MESH = pl.DeviceIdType.MESH


def transport(counts, pieces, steps, field, flow_j, flow_i, flow_k, end, mean_out, scale_out,
              cells, flows, face_out, face_in, stats, means,
              load_sem, flow_sem, end_sem, k_send, k_recv, i_send, i_recv, j_send, j_recv,
              stat_send, stat_recv):
    n_south, n_east, n_down = counts
    nj, ni, nk, _ = field.shape
    rows = nj // pieces
    south, east, down = (lax.axis_index(a) for a in ("south", "east", "down"))
    place = {"south": (south, n_south), "east": (east, n_east), "down": (down, n_down)}
    downward = lax.rem(south, 2) == 0

    def has(axis, side):
        me, count = place[axis]
        return me > 0 if side == 0 else me < count - 1

    def beside(axis, side):
        me, _ = place[axis]
        return {axis: me - 1 if side == 0 else me + 1}

    def piece_of(c):
        return jnp.where(downward, pieces - 1 - c, c)

    def load(c):
        return pltpu.make_async_copy(
            field.at[pl.ds(c * rows, rows)],
            cells.at[0, pl.ds(c * rows + 1, rows), pl.ds(1, ni)],
            load_sem.at[c],
        )

    def load_flow(d, c):
        source = (flow_j, flow_i, flow_k)[d]
        part = pl.ds(c * rows, rows)
        return pltpu.make_async_copy(source.at[part], flows.at[d, part], flow_sem.at[d, c])

    def k_copy(slot, side, c):
        part = pl.ds(c * rows, rows)
        return pltpu.make_async_remote_copy(
            face_out.at[slot, side, part], face_in.at[slot, 1 - side, part],
            k_send.at[slot, side, c], k_recv.at[slot, 1 - side, c],
            device_id=beside("down", side), device_id_type=MESH,
        )

    def i_copy(slot, side, c):
        part = pl.ds(c * rows + 1, rows)
        return pltpu.make_async_remote_copy(
            cells.at[slot, part, 1 if side == 0 else ni],
            cells.at[slot, part, ni + 1 if side == 0 else 0],
            i_send.at[slot, side, c], i_recv.at[slot, 1 - side, c],
            device_id=beside("east", side), device_id_type=MESH,
        )

    def j_copy(slot, side):
        return pltpu.make_async_remote_copy(
            cells.at[slot, 1 if side == 0 else nj, pl.ds(1, ni)],
            cells.at[slot, nj + 1 if side == 0 else 0, pl.ds(1, ni)],
            j_send.at[slot, side], j_recv.at[slot, 1 - side],
            device_id=beside("south", side), device_id_type=MESH,
        )

    def each_copy(slot, c, act):
        for side in (0, 1):
            pl.when(has("down", side))(lambda: act(k_copy(slot, side, c), side))
        for side in (0, 1):
            pl.when(has("east", side))(lambda: act(i_copy(slot, side, c), side))
        for side in (0, 1):
            edge = 0 if side == 0 else pieces - 1
            pl.when(has("south", side) & (c == edge))(lambda: act(j_copy(slot, side), side))

    def send(slot, c):
        each_copy(slot, c, lambda copy, side: copy.start())

    def sent(slot, c):
        each_copy(slot, c, lambda copy, side: copy.wait_send())

    def received(slot, c):
        for side in (0, 1):
            pl.when(has("down", side))(lambda: k_copy(slot, 1 - side, c).wait_recv())
        for side in (0, 1):
            pl.when(has("east", side))(lambda: i_copy(slot, 1 - side, c).wait_recv())
        for side in (0, 1):
            edge = 0 if side == 0 else pieces - 1
            pl.when(has("south", side) & (c == edge))(
                lambda: j_copy(slot, 1 - side).wait_recv()
            )

    barrier = pltpu.get_barrier_semaphore()
    for axis in ("east", "down"):
        for side in (0, 1):
            @pl.when(has(axis, side))
            def _():
                pl.semaphore_signal(barrier, 1, device_id=beside(axis, side), device_id_type=MESH)
    for offset in range(1, n_south):
        other = {"south": lax.rem(south + offset, n_south)}
        pl.semaphore_signal(barrier, 1, device_id=other, device_id_type=MESH)

    @pl.loop(0, pieces)
    def _(c):
        load(piece_of(c)).start()

    peers = n_south - 1
    for axis in ("east", "down"):
        for side in (0, 1):
            peers = peers + has(axis, side).astype(jnp.int32)
    pl.semaphore_wait(barrier, peers)

    @pl.loop(0, pieces)
    def _(index):
        c = piece_of(index)
        load(c).wait()

        @pl.loop(0, rows)
        def _(offset):
            r = c * rows + offset
            values = cells[0, r + 1, pl.ds(1, ni)]
            face_out[0, 0, r] = values[:, 0, :]
            face_out[0, 1, r] = values[:, nk - 1, :]

        send(0, c)
        for d in range(3):
            load_flow(d, c).start()

    for side in (0, 1):
        @pl.when(jnp.logical_not(has("down", side)))
        def _():
            @pl.loop(0, nj)
            def _(r):
                for slot in (0, 1):
                    face_in[slot, side, r] = jnp.zeros(face_in.shape[3:], jnp.float32)

        @pl.when(jnp.logical_not(has("east", side)))
        def _():
            @pl.loop(0, nj)
            def _(r):
                for slot in (0, 1):
                    cells[slot, r + 1, 0 if side == 0 else ni + 1] = jnp.zeros(
                        cells.shape[3:], jnp.float32)

        @pl.when(jnp.logical_not(has("south", side)))
        def _():
            for slot in (0, 1):
                cells[slot, 0 if side == 0 else nj + 1, pl.ds(1, ni)] = jnp.zeros(
                    field.shape[1:], jnp.float32)

    height = lax.broadcasted_iota(jnp.int32, field.shape[1:], 1)

    def advanced(slot, r):
        middle = cells[slot, r + 1, pl.ds(1, ni)]
        j_low = cells[slot, r, pl.ds(1, ni)]
        j_high = cells[slot, r + 2, pl.ds(1, ni)]
        i_low = cells[slot, r + 1, pl.ds(0, ni)]
        i_high = cells[slot, r + 1, pl.ds(2, ni)]
        k_low = jnp.where(
            height == 0, face_in[slot, 0, r][:, None, :], pltpu.roll(middle, 1, 1))
        k_high = jnp.where(
            height == nk - 1, face_in[slot, 1, r][:, None, :], pltpu.roll(middle, nk - 1, 1))
        spread = (j_low + j_high) + (i_low + i_high) + (k_low + k_high) - 6.0 * middle
        drift = (flows[0, r] * (j_high - j_low) + flows[1, r] * (i_high - i_low)
                 + flows[2, r] * (k_high - k_low))
        return middle - drift + 0.05 * spread

    @pl.loop(1, steps)
    def _(step):
        now, later = lax.rem(step + 1, 2), lax.rem(step, 2)

        @pl.loop(0, pieces)
        def _(index):
            c = piece_of(index)

            @pl.when(step == 1)
            def _():
                for d in range(3):
                    load_flow(d, c).wait()

            @pl.when(step >= 2)
            def _():
                sent(later, c)

            received(now, c)

            @pl.loop(0, rows)
            def _(offset):
                r = c * rows + offset
                values = advanced(now, r)
                cells[later, r + 1, pl.ds(1, ni)] = values
                face_out[later, 0, r] = values[:, 0, :]
                face_out[later, 1, r] = values[:, nk - 1, :]

            send(later, c)

    now, later = (steps - 1) % 2, steps % 2

    def store(c):
        return pltpu.make_async_copy(
            cells.at[later, pl.ds(c * rows + 1, rows), pl.ds(1, ni)],
            end.at[pl.ds(c * rows, rows)],
            end_sem.at[c],
        )

    def finish(index, squares):
        c = piece_of(index)
        sent(later, c)
        received(now, c)

        def row(offset, total):
            r = c * rows + offset
            values = advanced(now, r)
            cells[later, r + 1, pl.ds(1, ni)] = values
            return total + values

        own_mean = lax.fori_loop(0, rows, row, zero) * (1.0 / rows)
        store(c).start()
        means[index] = own_mean

        def square(offset, total):
            centred = cells[later, c * rows + offset + 1, pl.ds(1, ni)] - own_mean
            return total + centred * centred

        return lax.fori_loop(0, rows, square, squares)

    zero = jnp.zeros(field.shape[1:], jnp.float32)
    squares = lax.fori_loop(0, pieces, finish, zero)
    mean = means[0]
    for index in range(1, pieces):
        mean = mean + means[index]
    mean = mean * (1.0 / pieces)
    for index in range(pieces):
        away = means[index] - mean
        squares = squares + rows * (away * away)
    stats[south, 0] = mean
    stats[south, 1] = squares

    def stat_copy(offset, owner):
        target = lax.rem(south + offset, n_south)
        return pltpu.make_async_remote_copy(
            stats.at[owner], stats.at[owner], stat_send.at[offset - 1], stat_recv.at[offset - 1],
            device_id={"south": target}, device_id_type=MESH,
        )

    for offset in range(1, n_south):
        stat_copy(offset, south).start()

    @pl.loop(0, pieces)
    def _(c):
        sent(now, c)
        store(c).wait()

    for offset in range(1, n_south):
        owner = lax.rem(south + n_south - offset, n_south)
        stat_copy(offset, owner).wait_recv()
    whole_mean = stats[0, 0]
    for other in range(1, n_south):
        whole_mean = whole_mean + stats[other, 0]
    whole_mean = whole_mean * (1.0 / n_south)
    whole_squares = zero
    for other in range(n_south):
        away = stats[other, 0] - whole_mean
        whole_squares = whole_squares + (stats[other, 1] + nj * (away * away))
    mean_out[...] = whole_mean
    scale_out[...] = lax.rsqrt(whole_squares * (1.0 / (nj * n_south)) + 0.0001)
    for offset in range(1, n_south):
        stat_copy(offset, south).wait_send()


def scale(values, mean, factor, standardized, copied):
    block = values[...]
    copied[...] = block
    standardized[...] = (block - mean[...][None]) * factor[...][None]


def per_device(counts, field_values, flow_j, flow_i, flow_k):
    nj, ni, nk, levels = field_values.shape
    pieces = PIECES
    n_south = counts[0]
    plane = (ni, nk, levels)
    end, mean, factor = pl.pallas_call(
        functools.partial(transport, counts, pieces, STEPS),
        name="transport",
        out_shape=(
            jax.ShapeDtypeStruct(field_values.shape, jnp.float32),
            jax.ShapeDtypeStruct(plane, jnp.float32),
            jax.ShapeDtypeStruct(plane, jnp.float32),
        ),
        in_specs=[pl.BlockSpec(memory_space=pltpu.HBM)] * 4,
        out_specs=(
            pl.BlockSpec(memory_space=pl.ANY),
            pl.BlockSpec(memory_space=pltpu.VMEM),
            pl.BlockSpec(memory_space=pltpu.VMEM),
        ),
        scratch_shapes=[
            pltpu.VMEM((2, nj + 2, ni + 2, nk, levels), jnp.float32),
            pltpu.VMEM((3,) + field_values.shape, jnp.float32),
            pltpu.VMEM((2, 2, nj, ni, levels), jnp.float32),
            pltpu.VMEM((2, 2, nj, ni, levels), jnp.float32),
            pltpu.VMEM((n_south, 2) + plane, jnp.float32),
            pltpu.VMEM((pieces,) + plane, jnp.float32),
            pltpu.SemaphoreType.DMA((pieces,)),
            pltpu.SemaphoreType.DMA((3, pieces)),
            pltpu.SemaphoreType.DMA((pieces,)),
            pltpu.SemaphoreType.DMA((2, 2, pieces)),
            pltpu.SemaphoreType.DMA((2, 2, pieces)),
            pltpu.SemaphoreType.DMA((2, 2, pieces)),
            pltpu.SemaphoreType.DMA((2, 2, pieces)),
            pltpu.SemaphoreType.DMA((2, 2)),
            pltpu.SemaphoreType.DMA((2, 2)),
            pltpu.SemaphoreType.DMA((max(n_south - 1, 1),)),
            pltpu.SemaphoreType.DMA((max(n_south - 1, 1),)),
        ],
        compiler_params=pltpu.CompilerParams(
            collective_id=0, has_side_effects=True, vmem_limit_bytes=34 * 2**20
        ),
    )(*(pltpu.with_memory_space_constraint(array, pltpu.HBM)
        for array in (field_values, flow_j, flow_i, flow_k)))
    rows = nj // pieces
    block = pl.BlockSpec((rows,) + plane, lambda c: (c, 0, 0, 0))
    flat = pl.BlockSpec(plane, lambda c: (0, 0, 0))
    return pl.pallas_call(
        scale,
        name="scale",
        grid=(nj // rows,),
        in_specs=[block, flat, flat],
        out_specs=(block, block),
        out_shape=(jax.ShapeDtypeStruct(field_values.shape, jnp.float32),) * 2,
        compiler_params=pltpu.CompilerParams(vmem_limit_bytes=16 * 2**20),
    )(end, mean, factor)


def solution(mesh):
    counts = tuple(mesh.shape[axis] for axis in ("south", "east", "down"))
    spec = P("south", "east", "down", None)
    return jax.shard_map(
        functools.partial(per_device, counts),
        mesh=mesh,
        in_specs=(spec,) * 4,
        out_specs=(spec, spec),
        check_vma=False,
    )
```
